128 devices in a mesh: ctx: 8 (over z_lo, y), tp: 16 (over z_hi, x, core).
Axes of the slice: x: 4, y: 4, z: 4 (z_hi: 2, z_lo: 2; z = z_hi * 2 + z_lo), core: 2. Of those that a mesh axis runs over, the one named last changes fastest.
Arguments:
- queries: bfloat16 [8192, 8192], P('ctx', 'tp'), may hold values from -64 to 64
- context_keys: bfloat16 [8192, 1024], P('ctx'), may hold values from -6 to 6
- context_values: bfloat16 [8192, 1024], P('ctx'), may hold values from -6 to 6
- positions: int32 [8192], P('ctx'), may hold values from 0 to 8191, as said below
- out_weight: bfloat16 [8192, 8192], P('tp'), may hold values from -0.5 to 0.5
- residual_in: bfloat16 [8192, 8192], P(('ctx', 'tp')), may hold values from -3 to 3
- norm_gain: float32 [8192], replicated, may hold values from 0.5 to 1.5
- static_scale: float32 [1], replicated, may hold values from 0.004 to 0.009
Outputs:
- hidden_out: bfloat16 [8192, 8192], P(('ctx', 'tp'))
- clipped: bfloat16 [8192, 8192], P(('ctx', 'tp'))
The draws below stay inside these ranges and needn't reach their ends.
Inputs may be any that keep to these rules, and one draw needn't show every extreme that they name: Rows fall into aligned runs of 512 rows that hold consecutive positions in increasing order; all positions together are a permutation of 0 to 8191.
All inputs are finite; a program needn't handle non-finite values.
Results may differ from the reference program's by a relative error of at most 0.017.
Values may be sent and summed in bfloat16 or wider, within the bound.
A program may use at most 128 MiB of HBM per device.

```python
import math
import jax
import jax.numpy as jnp
from jax import lax

D = 8192
HEADS = 64
KVH = 8
HD = 128
TOK_DEV = 1024
SPAN = 512
TOKENS = 8192
N_TP = 16


def span_order(key):
    return jax.random.permutation(jax.random.fold_in(key, 5), TOKENS // SPAN).astype(jnp.int32)


def row_positions(key):
    order = span_order(key)
    row_ids = jnp.arange(TOKENS, dtype=jnp.int32)
    return (order[row_ids // SPAN] * SPAN + row_ids % SPAN).astype(jnp.int32)


def shared_draw(key):
    base_key = jax.random.fold_in(key, 71)
    first_key, second_key = jax.random.split(base_key, 2)
    key_table = jnp.clip(jax.random.normal(first_key, (TOKENS, KVH * HD), jnp.float32), -6.0, 6.0)
    query_table = jnp.clip(1.5 * jax.random.normal(second_key, (TOKENS, HEADS * HD), jnp.float32), -9.0, 9.0)
    return (query_table, key_table)


def draw_queries(key, part):
    return shared_draw(key)[0].astype(jnp.bfloat16)


def draw_context_keys(key, part):
    return shared_draw(key)[1].astype(jnp.bfloat16)


def draw_positions(key, part):
    return row_positions(key)


def shard_levels(stream_key, dims, pieces, least, high):
    level = 1.0
    for dim, shards_of in pieces:
        steps = jax.random.uniform(jax.random.fold_in(jax.random.fold_in(stream_key, 6), dim), (shards_of,), jnp.float32, least / len(pieces), high / len(pieces))
        level = level * jnp.repeat(jnp.exp(steps), dims[dim] // shards_of).reshape((-1,) + (1,) * (len(dims) - 1 - dim))
    return level


def scatter_about(stream_key, shape, spread, most, pieces=(), kind=jnp.bfloat16):
    level = shard_levels(stream_key, shape, pieces, -0.22, 0.18) if pieces else 1.0
    entries = jax.random.normal(stream_key, shape, jnp.float32) * spread * level
    return jnp.minimum(jnp.maximum(entries, -most), most).astype(kind)


def setup_inputs(seed: int = 0) -> dict:
    key_of = jax.random.split(jax.random.key(seed), 9)
    queries = draw_queries(jax.random.fold_in(key_of[8], 71), 0)
    context_keys = draw_context_keys(jax.random.fold_in(key_of[8], 71), 0)
    context_values = scatter_about(key_of[2], (TOKENS, KVH * HD), 1.0, 6.0, ((0, 8),))
    positions = draw_positions(jax.random.fold_in(key_of[8], 71), 0)
    out_weight = scatter_about(key_of[4], (HEADS * HD, D), HD ** -0.5, 0.5, ((0, 16),))
    residual_in = scatter_about(key_of[5], (TOKENS, D), 0.5, 3.0, ((0, 128),))
    norm_gain = jnp.clip(1.0 + 0.1 * jax.random.normal(key_of[6], (D,), jnp.float32), 0.5, 1.5)
    static_scale = jnp.clip(jnp.exp(jax.random.uniform(key_of[7], (1,), jnp.float32, math.log(0.004), math.log(0.009))), 0.004, 0.009)
    return dict(queries=queries, context_keys=context_keys, context_values=context_values, positions=positions, out_weight=out_weight, residual_in=residual_in, norm_gain=norm_gain, static_scale=static_scale)


masked_fill = -1e+30

def attend_head(head, queries, context_keys, context_values, positions):
    kv_head = head // (HEADS // KVH)
    query_cols = lax.dynamic_slice_in_dim(queries, head * HD, HD, 1).astype(jnp.float32)
    key_cols = lax.dynamic_slice_in_dim(context_keys, kv_head * HD, HD, 1).astype(jnp.float32)
    value_cols = lax.dynamic_slice_in_dim(context_values, kv_head * HD, HD, 1).astype(jnp.float32)
    block_count = TOKENS // TOK_DEV

    def one_block(block_args):
        query_blk, query_pos = block_args
        scores = jnp.dot(query_blk, key_cols.T, preferred_element_type=jnp.float32, precision=lax.Precision.HIGHEST) * (1.0 / math.sqrt(HD))
        allowed = positions[None, :] <= query_pos[:, None]
        row_max = lax.optimization_barrier(jnp.max(jnp.where(allowed, scores, masked_fill), axis=1))
        expo = jnp.where(allowed, jnp.exp(scores - row_max[:, None]), 0.0)
        row_total = lax.optimization_barrier(jnp.sum(expo, axis=1))
        rounded = lax.optimization_barrier(expo.astype(jnp.bfloat16))
        output = jnp.dot(rounded.astype(jnp.float32), value_cols, preferred_element_type=jnp.float32, precision=lax.Precision.HIGHEST)
        return (output / row_total[:, None]).astype(jnp.bfloat16)
    finished = lax.map(one_block, (query_cols.reshape(block_count, TOK_DEV, HD), positions.reshape(block_count, TOK_DEV)))
    return finished.reshape(TOKENS, HD)

def reference(queries, context_keys, context_values, positions, out_weight, residual_in, norm_gain, static_scale):
    head_ids = jnp.arange(HEADS, dtype=jnp.int32)
    attended = lax.map(lambda head: attend_head(head, queries, context_keys, context_values, positions), head_ids)
    attended = jnp.transpose(attended, (1, 0, 2)).reshape(TOKENS, HEADS * HD)
    group_width = HEADS * HD // N_TP
    summed = residual_in.astype(jnp.float32)
    for group_index in range(N_TP):
        low_col = group_index * group_width
        group_term = jnp.dot(attended[:, low_col:low_col + group_width].astype(jnp.float32), out_weight[low_col:low_col + group_width].astype(jnp.float32), preferred_element_type=jnp.float32, precision=lax.Precision.HIGHEST)
        group_term = lax.optimization_barrier(group_term.astype(jnp.bfloat16))
        summed = summed + group_term.astype(jnp.float32)
    hidden_out = summed.astype(jnp.bfloat16)
    inv_rms = lax.rsqrt(lax.optimization_barrier(jnp.mean(summed * summed, axis=1, keepdims=True)) + 1e-05)
    limit = 448.0 * static_scale[0]
    clipped = jnp.clip(summed * inv_rms * norm_gain[None, :], -limit, limit).astype(jnp.bfloat16)
    return (hidden_out, clipped)
```

```python
import math

import jax
import jax.numpy as jnp
from jax import lax
from jax.experimental import pallas as pl
from jax.experimental.pallas import tpu as pltpu
from jax.sharding import PartitionSpec as P

HD = 128
SPAN = 512
ROWS = 64
WIDTH = 8192
CHUNKS = 4
TILE = 512
NEG = -1e30
MESH = pl.DeviceIdType.MESH
bf16 = jnp.bfloat16
f32 = jnp.float32


def kernel(
    q_hbm, k_hbm, v_hbm, pos_hbm, w_hbm, res_hbm, gain_hbm, scale_ref,
    hidden_ref, clipped_ref,
    wbuf, kv, vt, qbuf, posall, qt, acc, m_sc, l_sc, att, send, recv, fin, zrecv, summed, res, gain,
    lsem, qsem, wsem, gs, gr, ds, dr, ps, pr, xs, xr, zs, zr,
):
    ctx = lax.axis_index("ctx")
    tp = lax.axis_index("tp")
    zlo, y = ctx // 4, ctx % 4
    zhi, x, core = tp // 8, (tp // 2) % 4, tp % 2
    group = tp // 2
    yup, ydn = (y + 1) % 4, (y + 3) % 4
    zother = 1 - zlo

    def at_ctx(zl, yy):
        return (zl * 4 + yy, tp)

    def at_tp(zh, xx, cc):
        return (ctx, zh * 8 + xx * 2 + cc)

    mate = at_tp(zhi, x, 1 - core)
    xup, xdn = at_tp(zhi, (x + 1) % 4, core), at_tp(zhi, (x + 3) % 4, core)
    zmate = at_tp(1 - zhi, x, core)

    def rcopy(src, dst, ssem, rsem, dev):
        return pltpu.make_async_remote_copy(
            src_ref=src, dst_ref=dst, send_sem=ssem, recv_sem=rsem, device_id=dev, device_id_type=MESH
        )

    load_k = pltpu.make_async_copy(
        k_hbm.at[:, :, pl.ds(pl.multiple_of(group * HD, HD), HD)], kv.at[0, pl.ds(2 * ctx, 2)], lsem.at[0]
    )
    load_v = pltpu.make_async_copy(
        v_hbm.at[:, :, pl.ds(pl.multiple_of(group * HD, HD), HD)], kv.at[1, pl.ds(2 * ctx, 2)], lsem.at[1]
    )
    load_p = pltpu.make_async_copy(pos_hbm, posall.at[ctx], lsem.at[2])
    qcol = pl.ds(pl.multiple_of(core * 512, 512), 512)
    load_q = pltpu.make_async_copy(q_hbm.at[:, core], qbuf.at[:, :, qcol], lsem.at[3])
    load_w = pltpu.make_async_copy(w_hbm, wbuf.at[core], lsem.at[4])
    load_r = pltpu.make_async_copy(res_hbm, res, lsem.at[5])
    load_g = pltpu.make_async_copy(gain_hbm, gain, lsem.at[6])
    for c in (load_k, load_v, load_p, load_q, load_w, load_r, load_g):
        c.start()

    barrier = pltpu.get_barrier_semaphore()
    peers = [mate, xup, xdn, zmate] + [((ctx + i) % 8, tp) for i in range(1, 8)]
    for dev in peers:
        pl.semaphore_signal(barrier, inc=1, device_id=dev, device_id_type=MESH)
    pl.semaphore_wait(barrier, len(peers))

    def item(what, zl, yy):
        return kv.at[what, pl.ds((zl * 4 + yy) * 2, 2)]

    def half(what, zl, yy, part):
        return kv.at[what, pl.ds((zl * 4 + yy) * 2 + part, 1)]

    started = []

    def start(copy):
        copy.start()
        started.append(copy)

    load_k.wait()
    load_v.wait()
    own = item(core, zlo, y)
    start(rcopy(own, own, gs.at[0], gr.at[0], at_ctx(zother, y)))
    start(rcopy(own, own, gs.at[1], gr.at[1], at_ctx(zlo, yup)))
    start(rcopy(own, own, gs.at[2], gr.at[2], at_ctx(zlo, ydn)))
    load_p.wait()
    for i in range(1, 8):
        start(rcopy(posall.at[ctx], posall.at[ctx], ps.at[i - 1], pr.at[i - 1], ((ctx + i) % 8, tp)))
    start(rcopy(q_hbm.at[:, 1 - core], qbuf.at[:, :, qcol], qsem.at[0], qsem.at[1], mate))
    start(rcopy(w_hbm, wbuf.at[core], wsem.at[0], wsem.at[1], mate))

    def arrived(ref, sem, dev):
        rcopy(ref, ref, gs.at[0], sem, dev).wait_recv()

    def pass_on(ref, n):
        start(rcopy(ref, ref, ds.at[n], dr.at[n], mate))

    got = item(core, zother, y)
    arrived(got, gr.at[0], mate)
    start(rcopy(got, got, gs.at[3], gr.at[3], at_ctx(zlo, yup)))
    start(rcopy(got, got, gs.at[4], gr.at[4], at_ctx(zlo, ydn)))
    pass_on(got, 0)
    for n, zl in ((1, zlo), (3, zother)):
        below, above = item(core, zl, ydn), item(core, zl, yup)
        arrived(below, gr.at[n], mate)
        h = half(core, zl, ydn, 0)
        start(rcopy(h, h, gs.at[n + 4], gr.at[n + 4], at_ctx(zlo, yup)))
        pass_on(below, n)
        arrived(above, gr.at[n + 1], mate)
        h = half(core, zl, yup, 1)
        start(rcopy(h, h, gs.at[n + 5], gr.at[n + 5], at_ctx(zlo, ydn)))
        pass_on(above, n + 1)
    yfar = (y + 2) % 4
    for n, zl in ((5, zlo), (7, zother)):
        for part in range(2):
            h = half(core, zl, yfar, part)
            arrived(h, gr.at[n + part], mate)
            pass_on(h, n + part)
    what = 1 - core
    arrived(item(what, zother, y), dr.at[0], mate)
    for n, zl in ((1, zlo), (3, zother)):
        arrived(item(what, zl, ydn), dr.at[n], mate)
        arrived(item(what, zl, yup), dr.at[n + 1], mate)
    for n, zl in ((5, zlo), (7, zother)):
        for part in range(2):
            arrived(half(what, zl, yfar, part), dr.at[n + part], mate)
    for i in range(1, 8):
        src = posall.at[(ctx + 8 - i) % 8]
        rcopy(src, src, ps.at[0], pr.at[i - 1], mate).wait_recv()
    load_q.wait()
    qother = qbuf.at[:, :, pl.ds(pl.multiple_of((1 - core) * 512, 512), 512)]
    rcopy(qother, qother, qsem.at[0], qsem.at[1], mate).wait_recv()

    @pl.loop(0, 16)
    def _(i):
        vt[i] = kv[1, i].T

    score_scale = math.log2(math.e) / math.sqrt(HD)

    def attend(tile, key_span, bias, first, diag):
        keys = kv[0, key_span]
        s = jnp.dot(
            jnp.concatenate([keys, keys], axis=1), qt[tile], preferred_element_type=f32
        )
        if diag is not None:
            s = jnp.where(diag, s, NEG)
        top = jnp.max(s, axis=0, keepdims=True)
        if first:
            new = top
            p = jnp.exp2(s - new)
            l_sc[tile] = jnp.sum(p, axis=0, keepdims=True)
            acc[tile] = jnp.dot(vt[key_span], p.astype(bf16), preferred_element_type=f32)
        else:
            old = m_sc[tile]
            new = jnp.maximum(old, top + bias)
            p = jnp.exp2(s - (new - bias))
            alpha = jnp.exp2(old - new)
            l_sc[tile] = l_sc[tile] * alpha + jnp.sum(p, axis=0, keepdims=True)
            acc[tile] = acc[tile] * alpha + jnp.dot(vt[key_span], p.astype(bf16), preferred_element_type=f32)
        m_sc[tile] = new

    def start_of(span):
        row = posall[span // 2, pl.ds(pl.multiple_of((span % 2) * 8, 8), 8), :][0:1]
        return jnp.concatenate([row, row], axis=1)

    own_spans = (2 * ctx, 2 * ctx + 1)
    own_starts = [start_of(span) for span in own_spans]

    def attention(dests):
        for tile in range(4):
            way, hh = tile // 2, tile % 2
            rows = qbuf[way * 4 + dests[way]]
            stack = jnp.concatenate(
                [rows[:, (hh * 4 + h) * HD : (hh * 4 + h + 1) * HD] for h in range(4)], axis=0
            )
            qf = stack.astype(f32).T * score_scale
            hi = qf.astype(bf16)
            lo = (qf - hi.astype(f32)).astype(bf16)
            qt[tile] = jnp.concatenate([hi, lo], axis=0)
        for tile in range(4):
            way = tile // 2
            key_at = lax.broadcasted_iota(jnp.int32, (SPAN, 256), 0)
            row_at = lax.broadcasted_iota(jnp.int32, (SPAN, 256), 1) % ROWS
            diag = key_at <= row_at + (dests[way] * 128 + core * ROWS)
            attend(tile, own_spans[way], None, True, diag)

        @pl.loop(1, 16)
        def _(i):
            for tile in range(4):
                way = tile // 2
                span = (own_spans[way] + i) % 16
                bias = jnp.where(start_of(span) < own_starts[way], 0.0, NEG).astype(f32)
                attend(tile, span, bias, False, None)

        for tile in range(4):
            way, hh = tile // 2, tile % 2
            out = (acc[tile] / l_sc[tile]).T.astype(bf16)
            for h in range(4):
                head = hh * 4 + h
                att[way * ROWS : (way + 1) * ROWS, head * HD : (head + 1) * HD] = out[h * ROWS : (h + 1) * ROWS]

    per = WIDTH // CHUNKS
    for step in range(4):
        dests = ((x + 3 - step) % 4, (x + 1 + step) % 4)
        attention(dests)
        if step == 0:
            load_w.wait()
            rcopy(w_hbm, wbuf.at[1 - core], wsem.at[0], wsem.at[1], mate).wait_recv()
        for chunk in range(CHUNKS):
            piece = pl.ds(chunk * per, per)
            if step > 0:
                for way in range(2):
                    r = recv.at[way, step - 1, :, piece]
                    rcopy(r, r, xs.at[0, 0, 0], xr.at[way, step - 1, chunk], mate).wait_recv()

            @pl.loop(0, per // TILE)
            def _(t):
                cols = pl.ds(pl.multiple_of(chunk * per + t * TILE, TILE), TILE)
                r = jnp.dot(att[:, :512], wbuf[0, :, cols], preferred_element_type=f32)
                r += jnp.dot(att[:, 512:], wbuf[1, :, cols], preferred_element_type=f32)
                up, down = r[:ROWS], r[ROWS:]
                if step > 0:
                    up += recv[0, step - 1, :, cols].astype(f32)
                    down += recv[1, step - 1, :, cols].astype(f32)
                if step < 3:
                    send[0, step, :, cols] = up.astype(bf16)
                    send[1, step, :, cols] = down.astype(bf16)
                else:
                    mine = zhi == 0
                    summed[:, cols] = jnp.where(mine, up, down)
                    fin[:, cols] = jnp.where(mine, down, up).astype(bf16)

            if step < 3:
                for way, dev in ((0, xup), (1, xdn)):
                    start(
                        rcopy(
                            send.at[way, step, :, piece], recv.at[way, step, :, piece],
                            xs.at[way, step, chunk], xr.at[way, step, chunk], dev,
                        )
                    )
            else:
                start(rcopy(fin.at[:, piece], zrecv.at[:, piece], zs.at[chunk], zr.at[chunk], zmate))

    load_r.wait()
    load_g.wait()
    squares = jnp.zeros((ROWS, TILE), f32)
    for chunk in range(CHUNKS):
        piece = zrecv.at[:, pl.ds(chunk * per, per)]
        rcopy(piece, piece, zs.at[0], zr.at[chunk], zmate).wait_recv()
        for t in range(per // TILE):
            cols = slice(chunk * per + t * TILE, chunk * per + (t + 1) * TILE)
            total = summed[:, cols] + zrecv[:, cols].astype(f32) + res[:, cols].astype(f32)
            summed[:, cols] = total
            hidden_ref[:, cols] = total.astype(bf16)
            squares += total * total
    inv_rms = lax.rsqrt(jnp.sum(squares, axis=1, keepdims=True) * (1.0 / WIDTH) + 1e-5)
    limit = 448.0 * scale_ref[0]
    for t in range(WIDTH // TILE):
        cols = slice(t * TILE, (t + 1) * TILE)
        value = summed[:, cols] * inv_rms * gain[:, cols]
        clipped_ref[:, cols] = jnp.minimum(jnp.maximum(value, -limit), limit).astype(bf16)
    for copy in started:
        copy.wait_send()


def shards(queries, context_keys, context_values, positions, out_weight, residual_in, norm_gain, static_scale):
    starts = jnp.broadcast_to(positions.reshape(2, SPAN)[:, :1, None], (2, 8, 128)).reshape(16, 128)
    dma = pltpu.SemaphoreType.DMA
    out = jax.ShapeDtypeStruct((ROWS, WIDTH), bf16)
    anywhere = pl.BlockSpec(memory_space=pl.ANY)
    return pl.pallas_call(
        kernel,
        out_shape=(out, out),
        in_specs=[anywhere] * 7 + [pl.BlockSpec(memory_space=pltpu.SMEM)],
        out_specs=(pl.BlockSpec(memory_space=pltpu.VMEM),) * 2,
        scratch_shapes=[
            pltpu.VMEM((2, 512, WIDTH), bf16),
            pltpu.VMEM((2, 16, SPAN, HD), bf16),
            pltpu.VMEM((16, HD, SPAN), bf16),
            pltpu.VMEM((8, ROWS, 1024), bf16),
            pltpu.VMEM((8, 16, 128), jnp.int32),
            pltpu.VMEM((4, 2 * HD, 256), bf16),
            pltpu.VMEM((4, HD, 256), f32),
            pltpu.VMEM((4, 1, 256), f32),
            pltpu.VMEM((4, 1, 256), f32),
            pltpu.VMEM((2 * ROWS, 1024), bf16),
            pltpu.VMEM((2, 3, ROWS, WIDTH), bf16),
            pltpu.VMEM((2, 3, ROWS, WIDTH), bf16),
            pltpu.VMEM((ROWS, WIDTH), bf16),
            pltpu.VMEM((ROWS, WIDTH), bf16),
            pltpu.VMEM((ROWS, WIDTH), f32),
            pltpu.VMEM((ROWS, WIDTH), bf16),
            pltpu.VMEM((1, WIDTH), f32),
            dma((7,)), dma((2,)), dma((2,)), dma((9,)), dma((9,)), dma((9,)), dma((9,)), dma((7,)), dma((7,)),
            dma((2, 3, CHUNKS)), dma((2, 3, CHUNKS)), dma((CHUNKS,)), dma((CHUNKS,)),
        ],
        compiler_params=pltpu.CompilerParams(
            collective_id=0, has_side_effects=True, vmem_limit_bytes=62 * 1024 * 1024
        ),
    )(
        queries.reshape(8, 2, ROWS, 512),
        context_keys.reshape(2, SPAN, 1024),
        context_values.reshape(2, SPAN, 1024),
        starts,
        out_weight,
        residual_in,
        norm_gain.reshape(1, WIDTH),
        static_scale,
    )


def solution(mesh):
    return jax.shard_map(
        shards,
        mesh=mesh,
        in_specs=(
            P("ctx", "tp"),
            P("ctx", None),
            P("ctx", None),
            P("ctx"),
            P("tp", None),
            P(("ctx", "tp"), None),
            P(),
            P(),
        ),
        out_specs=(P(("ctx", "tp"), None), P(("ctx", "tp"), None)),
        check_vma=False,
    )
```

```python
import math

import jax
import jax.numpy as jnp
from jax import lax
from jax.experimental import pallas as pl
from jax.experimental.pallas import tpu as pltpu
from jax.sharding import PartitionSpec as P

HD = 128
SPAN = 512
ROWS = 64
WIDTH = 8192
TILE = 512
A_COLS = 5120
A_CHUNKS = 5
A_PER = A_COLS // A_CHUNKS
B_COLS = (WIDTH - A_COLS) // 2
NEG = -1e30
MESH = pl.DeviceIdType.MESH
bf16 = jnp.bfloat16
f32 = jnp.float32


def kernel(
    q_hbm, k_hbm, v_hbm, pos_hbm, w_hbm, res_hbm, gain_hbm, scale_ref,
    hidden_ref, clipped_ref,
    wbuf, kv, foreign, vt, qbuf, posall, qt, acc, m_sc, a_sc, t_sc, s_sc, p_sc, att,
    send, recv, zsend, zgot, bown, bsend, brecv, fin, zrecv, summed, res, gain,
    lsem, qsem, wsem, gs, gr, ds, dr, ps, pr, xs, xr, bzs, bzr, bxs, bxr, zs, zr,
):
    ctx = lax.axis_index("ctx")
    tp = lax.axis_index("tp")
    zlo, y = ctx // 4, ctx % 4
    zhi, x, core = tp // 8, (tp // 2) % 4, tp % 2
    group = tp // 2
    yup, ydn, yfar = (y + 1) % 4, (y + 3) % 4, (y + 2) % 4
    zother = 1 - zlo

    def at_ctx(zl, yy):
        return (zl * 4 + yy, tp)

    def at_tp(zh, xx, cc):
        return (ctx, zh * 8 + xx * 2 + cc)

    mate = at_tp(zhi, x, 1 - core)
    xup, xdn = at_tp(zhi, (x + 1) % 4, core), at_tp(zhi, (x + 3) % 4, core)
    zmate = at_tp(1 - zhi, x, core)
    zpair = at_ctx(zother, y)
    znext = (zother * 4 + y, (1 - zhi) * 8 + x * 2 + core)
    yabove, ybelow = at_ctx(zlo, yup), at_ctx(zlo, ydn)

    def rcopy(src, dst, ssem, rsem, dev):
        return pltpu.make_async_remote_copy(
            src_ref=src, dst_ref=dst, send_sem=ssem, recv_sem=rsem, device_id=dev, device_id_type=MESH
        )

    def heads(g):
        return pl.ds(pl.multiple_of(g * HD, HD), HD)

    far_group = (1 - zhi) * 4 + x
    qcol = pl.ds(pl.multiple_of(core * 512, 512), 512)
    loads = []
    for n, (source, target) in enumerate((
        (k_hbm.at[:, :, heads(group)], kv.at[0, pl.ds(2 * ctx, 2)]),
        (v_hbm.at[:, :, heads(group)], kv.at[1, pl.ds(2 * ctx, 2)]),
        (k_hbm.at[pl.ds(1, 1), :, heads(far_group)], foreign.at[0]),
        (v_hbm.at[pl.ds(1, 1), :, heads(far_group)], foreign.at[1]),
        (pos_hbm, posall.at[ctx]),
        (q_hbm.at[:, core], qbuf.at[:, :, qcol]),
        (w_hbm, wbuf.at[core]),
        (res_hbm, res),
        (gain_hbm, gain),
    )):
        copy = pltpu.make_async_copy(source, target, lsem.at[n])
        copy.start()
        loads.append(copy)

    barrier = pltpu.get_barrier_semaphore()
    peers = [mate, xup, xdn, zmate, znext] + [((ctx + i) % 8, tp) for i in range(1, 8)]
    for dev in peers:
        pl.semaphore_signal(barrier, inc=1, device_id=dev, device_id_type=MESH)
    pl.semaphore_wait(barrier, len(peers))

    def item(what, zl, yy):
        return kv.at[what, pl.ds((zl * 4 + yy) * 2, 2)]

    def half(what, zl, yy, part):
        return kv.at[what, pl.ds((zl * 4 + yy) * 2 + part, 1)]

    started = []

    def start(copy):
        copy.start()
        started.append(copy)

    waiting = [5, 6, 0, 1, 2, 3, 4, 7]

    def weights_on(count):
        for _ in range(count):
            if waiting:
                n = waiting.pop(0)
                piece = pl.ds(n * 1024, 1024)
                start(rcopy(w_hbm.at[:, piece], wbuf.at[core, :, piece], wsem.at[0, n], wsem.at[1, n], mate))

    here = set()

    def weights_here(*pieces):
        for n in pieces:
            if n not in here:
                here.add(n)
                arrived(wbuf.at[1 - core, :, pl.ds(n * 1024, 1024)], wsem.at[1, n])

    def send_on(ref, n, dev):
        start(rcopy(ref, ref, gs.at[n], gr.at[n], dev))

    def arrived(ref, sem):
        rcopy(ref, ref, gs.at[0], sem, mate).wait_recv()

    def pass_on(ref, n):
        start(rcopy(ref, ref, ds.at[n], dr.at[n], mate))

    for n in range(4):
        loads[n].wait()
    first = half(core, zlo, y, 0)
    send_on(first, 0, zpair)
    start(rcopy(foreign.at[core], half(core, zlo, y, 1), gs.at[1], gr.at[1], znext))
    own = item(core, zlo, y)
    send_on(own, 2, yabove)
    send_on(own, 3, ybelow)
    start(rcopy(q_hbm.at[:, 1 - core], qbuf.at[:, :, qcol], qsem.at[0], qsem.at[1], mate))
    loads[4].wait()
    for i in range(1, 8):
        start(rcopy(posall.at[ctx], posall.at[ctx], ps.at[i - 1], pr.at[i - 1], ((ctx + i) % 8, tp)))
    weights_on(2)

    order = [
        zlo * 4 + y, zother * 4 + y, zlo * 4 + ydn, zlo * 4 + yup,
        zother * 4 + ydn, zother * 4 + yup, zlo * 4 + yfar, zother * 4 + yfar,
    ]

    def gathered(n):
        if n == 1:
            got = half(core, zother, y, 1)
            arrived(got, gr.at[1])
            send_on(got, 4, yabove)
            send_on(got, 5, ybelow)
            pass_on(got, 1)
            got = half(core, zother, y, 0)
            arrived(got, gr.at[0])
            pass_on(got, 0)
            weights_on(1)
        elif n == 2:
            got = item(core, zlo, ydn)
            arrived(got, gr.at[2])
            send_on(half(core, zlo, ydn, 0), 6, yabove)
            send_on(half(core, zlo, ydn, 0), 7, zpair)
            pass_on(got, 2)
            got = item(core, zlo, yup)
            arrived(got, gr.at[3])
            send_on(half(core, zlo, yup, 1), 8, ybelow)
            send_on(half(core, zlo, yup, 0), 9, zpair)
            pass_on(got, 3)
            weights_on(2)
        elif n == 4:
            below, above = half(core, zother, ydn, 1), half(core, zother, yup, 1)
            arrived(below, gr.at[4])
            arrived(above, gr.at[5])
            lower = core == 0
            source = jnp.where(lower, ydn, yup)
            target = at_ctx(zlo, jnp.where(lower, yup, ydn))
            send_on(half(core, zother, source, 1), 10, target)
            pass_on(below, 4)
            pass_on(above, 5)
            got = half(core, zlo, yfar, 0)
            arrived(got, gr.at[6])
            send_on(got, 11, zpair)
            pass_on(got, 6)
            got = half(core, zlo, yfar, 1)
            arrived(got, gr.at[8])
            pass_on(got, 8)
            weights_on(1)
        elif n == 5:
            got = half(core, zother, ydn, 0)
            arrived(got, gr.at[7])
            pass_on(got, 7)
            got = half(core, zother, yup, 0)
            arrived(got, gr.at[9])
            pass_on(got, 9)
            weights_on(2)
        elif n == 7:
            got = half(core, zother, yfar, 1)
            arrived(got, gr.at[10])
            pass_on(got, 10)
            got = half(core, zother, yfar, 0)
            arrived(got, gr.at[11])
            pass_on(got, 11)

    def ready(n):
        what = 1 - core
        if n == 1:
            arrived(half(what, zother, y, 1), dr.at[1])
            arrived(half(what, zother, y, 0), dr.at[0])
        elif n == 2:
            arrived(item(what, zlo, ydn), dr.at[2])
        elif n == 3:
            arrived(item(what, zlo, yup), dr.at[3])
        elif n == 4:
            arrived(half(what, zother, ydn, 1), dr.at[4])
            arrived(half(what, zother, ydn, 0), dr.at[7])
        elif n == 5:
            arrived(half(what, zother, yup, 1), dr.at[5])
            arrived(half(what, zother, yup, 0), dr.at[9])
        elif n == 6:
            arrived(half(what, zlo, yfar, 0), dr.at[6])
            arrived(half(what, zlo, yfar, 1), dr.at[8])
        elif n == 7:
            arrived(half(what, zother, yfar, 1), dr.at[10])
            arrived(half(what, zother, yfar, 0), dr.at[11])
        for part in range(2):
            span = order[n] * 2 + part
            vt[span, :HD] = kv[1, span].T

    vt[:, HD:] = jnp.ones((16, 16, SPAN), bf16)

    score_scale = math.log2(math.e) / math.sqrt(HD)

    def fold(scores):
        return jnp.max(scores.reshape(SPAN // 8, 8, 256), axis=0)

    def scores_of(tile, key_span):
        keys = kv[0, key_span]
        keys = jnp.concatenate([keys, keys], axis=1)
        parts = [
            jnp.dot(keys[h * 256 : (h + 1) * 256], qt[tile], preferred_element_type=f32) for h in range(2)
        ]
        return jnp.concatenate(parts, axis=0)

    def start_of(span):
        row = posall[span // 2, pl.ds(pl.multiple_of((span % 2) * 8, 8), 8), :][0:1]
        return jnp.concatenate([row, row], axis=1)

    own_spans = (2 * ctx, 2 * ctx + 1)

    def attention(place, dests, during_gather):
        own_starts = [start_of(span) for span in own_spans]
        for tile in range(4):
            way, hh = tile // 2, tile % 2
            rows = qbuf[way * 4 + dests[way]]
            stack = jnp.concatenate(
                [rows[:, (hh * 4 + h) * HD : (hh * 4 + h + 1) * HD] for h in range(4)], axis=0
            )
            qf = stack.astype(f32).T * score_scale
            hi = qf.astype(bf16)
            lo = (qf - hi.astype(f32)).astype(bf16)
            qt[tile] = jnp.concatenate([hi, lo], axis=0)

        def masked(tile, s):
            key_at = lax.broadcasted_iota(jnp.int32, (SPAN, 256), 0)
            row_at = lax.broadcasted_iota(jnp.int32, (SPAN, 256), 1) % ROWS
            return jnp.where(key_at <= row_at + (dests[tile // 2] * 128 + core * ROWS), s, NEG)

        def span_at(tile, i):
            way = tile // 2
            if during_gather:
                return order[i // 2 % 8] * 2 + (i % 2 if way == 0 else 1 - i % 2)
            return (own_spans[way] + i) % 16

        def product(tile, i, slot):
            r = jnp.dot(vt[span_at(tile, i)], p_sc[slot], preferred_element_type=f32)[: HD + 8]
            acc[tile] = acc[tile] * a_sc[slot] + r

        def units(i, own):
            for tile in range(4):
                cur, nxt = tile % 2, (tile + 1) % 2
                after, ai = (tile + 1) % 4, i + (tile + 1) // 4
                before, bi = (tile + 3) % 4, i - (1 if tile == 0 else 0)
                last = during_gather and i == 15 and tile == 3
                top = jnp.max(t_sc[cur], axis=0, keepdims=True)
                old = m_sc[tile]
                if own:
                    new = offset = jnp.maximum(old, top)
                else:
                    visible = start_of(span_at(tile, i)) < own_starts[tile // 2]
                    bias = jnp.where(visible, 0.0, NEG).astype(f32)
                    new = jnp.maximum(old, top + bias)
                    offset = new - bias
                m_sc[tile] = new
                if not last:
                    s = scores_of(after, span_at(after, ai))
                    if own and tile < 3:
                        s = masked(after, s)
                if not (own and tile == 0):
                    product(before, bi, nxt)
                a_sc[cur] = jnp.exp2(old - new)
                tops = None
                for sub in range(4):
                    rows = slice(sub * 128, (sub + 1) * 128)
                    if not last:
                        s_sc[nxt, rows] = s[rows]
                        t = jnp.max(s[rows].reshape(16, 8, 256), axis=0)
                        tops = t if tops is None else jnp.maximum(tops, t)
                    p_sc[cur, rows] = jnp.exp2(s_sc[cur, rows] - offset).astype(bf16)
                if not last:
                    t_sc[nxt] = tops

        for tile in range(4):
            m_sc[tile] = jnp.full((1, 256), NEG, f32)
            acc[tile] = jnp.zeros((HD + 8, 256), f32)
        if during_gather:
            ready(0)
        s = masked(0, scores_of(0, own_spans[0]))
        s_sc[0] = s
        t_sc[0] = fold(s)
        if during_gather:
            gathered(1)
            units(0, True)
            for i in range(1, 8):
                src = posall.at[(ctx + 8 - i) % 8]
                rcopy(src, src, ps.at[0], pr.at[i - 1], mate).wait_recv()
            gathered(2)
            for n in range(8):
                if n in (2, 3, 5):
                    gathered({2: 4, 3: 5, 5: 7}[n])
                if n < 7:
                    ready(n + 1)
                for i in range(max(2 * n, 1), 2 * n + 2):
                    units(i, False)
        else:
            units(0, True)

            @pl.loop(1, 16)
            def _(i):
                units(i, False)

        product(3, 15, 1)

        for tile in range(4):
            way, hh = tile // 2, tile % 2
            out = (acc[tile, :HD] / acc[tile, HD : HD + 1]).T.astype(bf16)
            for h in range(4):
                head = hh * 4 + h
                att[place, way * ROWS : (way + 1) * ROWS, head * HD : (head + 1) * HD] = out[
                    h * ROWS : (h + 1) * ROWS
                ]

    def projected(place, cols):
        r = jnp.dot(att[place, :, :512], wbuf[0, :, cols], preferred_element_type=f32)
        return r + jnp.dot(att[place, :, 512:], wbuf[1, :, cols], preferred_element_type=f32)

    mine = zhi == 0

    def across(step, place):
        for chunk in range(A_CHUNKS):
            piece = pl.ds(chunk * A_PER, A_PER)
            if step == 0:
                weights_here(chunk)
            if step > 0:
                for way in range(2):
                    arrived(recv.at[way, step - 1, :, piece], xr.at[way, step - 1, chunk])

            @pl.loop(0, A_PER // TILE)
            def _(t):
                cols = pl.ds(pl.multiple_of(chunk * A_PER + t * TILE, TILE), TILE)
                r = projected(place, cols)
                up, down = r[:ROWS], r[ROWS:]
                if step > 0:
                    up += recv[0, step - 1, :, cols].astype(f32)
                    down += recv[1, step - 1, :, cols].astype(f32)
                if step < 3:
                    send[0, step, :, cols] = up.astype(bf16)
                    send[1, step, :, cols] = down.astype(bf16)
                else:
                    summed[:, cols] = jnp.where(mine, up, down)
                    fin[:, cols] = jnp.where(mine, down, up).astype(bf16)

            if step < 3:
                for way, dev in ((0, xup), (1, xdn)):
                    start(
                        rcopy(
                            send.at[way, step, :, piece], recv.at[way, step, :, piece],
                            xs.at[way, step, chunk], xr.at[way, step, chunk], dev,
                        )
                    )
            else:
                start(rcopy(fin.at[:, piece], zrecv.at[:, piece], zs.at[chunk], zr.at[chunk], zmate))

    def begin(ring, step, place):
        weights_here(*((5, 6) if ring == 0 else (6, 7)))

        @pl.loop(0, B_COLS // TILE)
        def _(t):
            cols = pl.ds(pl.multiple_of(t * TILE, TILE), TILE)
            r = projected(
                place, pl.ds(pl.multiple_of(A_COLS + ring * B_COLS + t * TILE, TILE), TILE)
            )
            bown[ring, step, :, cols] = jnp.where(mine, r[:ROWS], r[ROWS:])
            zsend[ring, step, :, cols] = jnp.where(mine, r[ROWS:], r[:ROWS]).astype(bf16)

        start(
            rcopy(
                zsend.at[ring, step], zgot.at[ring, step], bzs.at[ring, step], bzr.at[ring, step], zmate
            )
        )

    def finish(ring, step):
        arrived(zgot.at[ring, step], bzr.at[ring, step])
        if step > 0:
            arrived(brecv.at[ring, step - 1], bxr.at[ring, step - 1])

        @pl.loop(0, B_COLS // TILE)
        def _(t):
            cols = pl.ds(pl.multiple_of(t * TILE, TILE), TILE)
            v = bown[ring, step, :, cols] + zgot[ring, step, :, cols].astype(f32)
            if step > 0:
                v += brecv[ring, step - 1, :, cols].astype(f32)
            if step < 3:
                bsend[ring, step, :, cols] = v.astype(bf16)
            else:
                summed[:, pl.ds(pl.multiple_of(A_COLS + ring * B_COLS + t * TILE, TILE), TILE)] = v

        if step < 3:
            ahead = (x + jnp.where((zhi + ring) % 2 == 0, 1, 3)) % 4
            start(
                rcopy(
                    bsend.at[ring, step], brecv.at[ring, step], bxs.at[ring, step], bxr.at[ring, step],
                    at_tp(zhi, ahead, core),
                )
            )

    left, right, far = (x + 3) % 4, (x + 1) % 4, (x + 2) % 4
    loads[5].wait()
    qother = qbuf.at[:, :, pl.ds(pl.multiple_of((1 - core) * 512, 512), 512)]
    arrived(qother, qsem.at[1])
    attention(0, (left, right), True)
    weights_on(8)
    loads[6].wait()
    begin(0, 0, 0)
    across(0, 0)
    begin(1, 2, 0)
    attention(1, (far, far), False)
    finish(0, 0)
    begin(0, 1, 1)
    begin(1, 1, 1)
    across(1, 1)
    attention(2, (right, left), False)
    begin(1, 0, 2)
    begin(0, 2, 2)
    finish(0, 1)
    finish(1, 0)
    across(2, 2)
    attention(3, (x, x), False)
    begin(0, 3, 3)
    begin(1, 3, 3)
    finish(0, 2)
    finish(1, 1)
    across(3, 3)
    finish(0, 3)
    finish(1, 2)
    finish(1, 3)

    loads[7].wait()
    loads[8].wait()
    squares = jnp.zeros((ROWS, TILE), f32)

    def total_of(start_col, crossed):
        cols = slice(start_col, start_col + TILE)
        total = summed[:, cols] + res[:, cols].astype(f32)
        if crossed:
            total += zrecv[:, cols].astype(f32)
        summed[:, cols] = total
        hidden_ref[:, cols] = total.astype(bf16)
        return total * total

    for t in range(A_COLS, WIDTH, TILE):
        squares += total_of(t, False)
    for chunk in range(A_CHUNKS):
        arrived(zrecv.at[:, pl.ds(chunk * A_PER, A_PER)], zr.at[chunk])
        for t in range(chunk * A_PER, (chunk + 1) * A_PER, TILE):
            squares += total_of(t, True)
    inv_rms = lax.rsqrt(jnp.sum(squares, axis=1, keepdims=True) * (1.0 / WIDTH) + 1e-5)
    limit = 448.0 * scale_ref[0]
    for t in range(WIDTH // TILE):
        cols = slice(t * TILE, (t + 1) * TILE)
        value = summed[:, cols] * inv_rms * gain[:, cols]
        clipped_ref[:, cols] = jnp.minimum(jnp.maximum(value, -limit), limit).astype(bf16)
    for copy in started:
        copy.wait_send()


def shards(queries, context_keys, context_values, positions, out_weight, residual_in, norm_gain, static_scale):
    starts = jnp.broadcast_to(positions.reshape(2, SPAN)[:, :1, None], (2, 8, 128)).reshape(16, 128)
    dma = pltpu.SemaphoreType.DMA
    out = jax.ShapeDtypeStruct((ROWS, WIDTH), bf16)
    anywhere = pl.BlockSpec(memory_space=pl.ANY)
    return pl.pallas_call(
        kernel,
        out_shape=(out, out),
        in_specs=[anywhere] * 7 + [pl.BlockSpec(memory_space=pltpu.SMEM)],
        out_specs=(pl.BlockSpec(memory_space=pltpu.VMEM),) * 2,
        scratch_shapes=[
            pltpu.VMEM((2, 512, WIDTH), bf16),
            pltpu.VMEM((2, 16, SPAN, HD), bf16),
            pltpu.VMEM((2, 1, SPAN, HD), bf16),
            pltpu.VMEM((16, HD + 16, SPAN), bf16),
            pltpu.VMEM((8, ROWS, 1024), bf16),
            pltpu.VMEM((8, 16, 128), jnp.int32),
            pltpu.VMEM((4, 2 * HD, 256), bf16),
            pltpu.VMEM((4, HD + 8, 256), f32),
            pltpu.VMEM((4, 1, 256), f32),
            pltpu.VMEM((2, 1, 256), f32),
            pltpu.VMEM((2, 8, 256), f32),
            pltpu.VMEM((2, SPAN, 256), f32),
            pltpu.VMEM((2, SPAN, 256), bf16),
            pltpu.VMEM((4, 2 * ROWS, 1024), bf16),
            pltpu.VMEM((2, 3, ROWS, A_COLS), bf16),
            pltpu.VMEM((2, 3, ROWS, A_COLS), bf16),
            pltpu.VMEM((2, 4, ROWS, B_COLS), bf16),
            pltpu.VMEM((2, 4, ROWS, B_COLS), bf16),
            pltpu.VMEM((2, 4, ROWS, B_COLS), f32),
            pltpu.VMEM((2, 3, ROWS, B_COLS), bf16),
            pltpu.VMEM((2, 3, ROWS, B_COLS), bf16),
            pltpu.VMEM((ROWS, A_COLS), bf16),
            pltpu.VMEM((ROWS, A_COLS), bf16),
            pltpu.VMEM((ROWS, WIDTH), f32),
            pltpu.VMEM((ROWS, WIDTH), bf16),
            pltpu.VMEM((1, WIDTH), f32),
            dma((9,)), dma((2,)), dma((2, 8)), dma((12,)), dma((12,)), dma((12,)), dma((12,)), dma((7,)), dma((7,)),
            dma((2, 3, A_CHUNKS)), dma((2, 3, A_CHUNKS)), dma((2, 4)), dma((2, 4)), dma((2, 3)), dma((2, 3)),
            dma((A_CHUNKS,)), dma((A_CHUNKS,)),
        ],
        compiler_params=pltpu.CompilerParams(
            collective_id=0, has_side_effects=True, vmem_limit_bytes=62 * 1024 * 1024
        ),
    )(
        queries.reshape(8, 2, ROWS, 512),
        context_keys.reshape(2, SPAN, 1024),
        context_values.reshape(2, SPAN, 1024),
        starts,
        out_weight,
        residual_in,
        norm_gain.reshape(1, WIDTH),
        static_scale,
    )


def solution(mesh):
    return jax.shard_map(
        shards,
        mesh=mesh,
        in_specs=(
            P("ctx", "tp"),
            P("ctx", None),
            P("ctx", None),
            P("ctx"),
            P("tp", None),
            P(("ctx", "tp"), None),
            P(),
            P(),
        ),
        out_specs=(P(("ctx", "tp"), None), P(("ctx", "tp"), None)),
        check_vma=False,
    )
```

```python
import math

import jax
import jax.numpy as jnp
from jax import lax
from jax.experimental import pallas as pl
from jax.experimental.pallas import tpu as pltpu
from jax.sharding import PartitionSpec as P

HD = 128
SPAN = 512
ROWS = 64
WIDTH = 8192
TILE = 512
NORM_ROWS = 16
A_TILE = 1024
B_TILE = 1536
A_COLS = 5120
A_CHUNKS = 5
A_PER = A_COLS // A_CHUNKS
B_COLS = (WIDTH - A_COLS) // 2
NEG = -1e30
MESH = pl.DeviceIdType.MESH
bf16 = jnp.bfloat16
f32 = jnp.float32


def kernel(
    q_hbm, k_hbm, v_hbm, pos_hbm, w_hbm, res_hbm,
    total_hbm,
    wbuf, kv, foreign, vt, qbuf, posall, qt, acc, m_sc, a_sc, t_sc, s_sc, p_sc, att,
    send, recv, zsend, zgot, bown, bsend, brecv, fin, zrecv, summed, res,
    lsem, tsem, qsem, wsem, gs, gr, ds, dr, ps, pr, xs, xr, bzs, bzr, bxs, bxr, zs, zr,
):
    ctx = lax.axis_index("ctx")
    tp = lax.axis_index("tp")
    zlo, y = ctx // 4, ctx % 4
    zhi, x, core = tp // 8, (tp // 2) % 4, tp % 2
    group = tp // 2
    yup, ydn, yfar = (y + 1) % 4, (y + 3) % 4, (y + 2) % 4
    zother = 1 - zlo

    def at_ctx(zl, yy):
        return (zl * 4 + yy, tp)

    def at_tp(zh, xx, cc):
        return (ctx, zh * 8 + xx * 2 + cc)

    mate = at_tp(zhi, x, 1 - core)
    xup, xdn = at_tp(zhi, (x + 1) % 4, core), at_tp(zhi, (x + 3) % 4, core)
    zmate = at_tp(1 - zhi, x, core)
    zpair = at_ctx(zother, y)
    znext = (zother * 4 + y, (1 - zhi) * 8 + x * 2 + core)
    yabove, ybelow = at_ctx(zlo, yup), at_ctx(zlo, ydn)

    def rcopy(src, dst, ssem, rsem, dev):
        return pltpu.make_async_remote_copy(
            src_ref=src, dst_ref=dst, send_sem=ssem, recv_sem=rsem, device_id=dev, device_id_type=MESH
        )

    def heads(g):
        return pl.ds(pl.multiple_of(g * HD, HD), HD)

    far_group = (1 - zhi) * 4 + x
    qcol = pl.ds(pl.multiple_of(core * 512, 512), 512)
    loads = []
    for n, (source, target) in enumerate((
        (k_hbm.at[:, :, heads(group)], kv.at[0, pl.ds(2 * ctx, 2)]),
        (v_hbm.at[:, :, heads(group)], kv.at[1, pl.ds(2 * ctx, 2)]),
        (k_hbm.at[pl.ds(1, 1), :, heads(far_group)], foreign.at[0]),
        (v_hbm.at[pl.ds(1, 1), :, heads(far_group)], foreign.at[1]),
        (pos_hbm, posall.at[ctx]),
        (q_hbm.at[:, core], qbuf.at[:, :, qcol]),
        (w_hbm, wbuf.at[core]),
        (res_hbm, res),
    )):
        copy = pltpu.make_async_copy(source, target, lsem.at[n])
        copy.start()
        loads.append(copy)

    barrier = pltpu.get_barrier_semaphore()
    peers = [mate, xup, xdn, zmate, znext] + [((ctx + i) % 8, tp) for i in range(1, 8)]
    for dev in peers:
        pl.semaphore_signal(barrier, inc=1, device_id=dev, device_id_type=MESH)
    pl.semaphore_wait(barrier, len(peers))

    def item(what, zl, yy):
        return kv.at[what, pl.ds((zl * 4 + yy) * 2, 2)]

    def half(what, zl, yy, part):
        return kv.at[what, pl.ds((zl * 4 + yy) * 2 + part, 1)]

    started = []

    def start(copy):
        copy.start()
        started.append(copy)

    waiting = [5, 6, 0, 1, 2, 3, 4, 7]

    def weights_on(count):
        for _ in range(count):
            if waiting:
                n = waiting.pop(0)
                piece = pl.ds(n * 1024, 1024)
                start(rcopy(w_hbm.at[:, piece], wbuf.at[core, :, piece], wsem.at[0, n], wsem.at[1, n], mate))

    here = set()

    def weights_here(*pieces):
        for n in pieces:
            if n not in here:
                here.add(n)
                arrived(wbuf.at[1 - core, :, pl.ds(n * 1024, 1024)], wsem.at[1, n])

    def send_on(ref, n, dev):
        start(rcopy(ref, ref, gs.at[n], gr.at[n], dev))

    def arrived(ref, sem):
        rcopy(ref, ref, gs.at[0], sem, mate).wait_recv()

    def pass_on(ref, n):
        start(rcopy(ref, ref, ds.at[n], dr.at[n], mate))

    loads[4].wait()
    for i in range(1, 8):
        start(rcopy(posall.at[ctx], posall.at[ctx], ps.at[i - 1], pr.at[i - 1], ((ctx + i) % 8, tp)))
    for n in range(4):
        loads[n].wait()
    first = half(core, zlo, y, 0)
    send_on(first, 0, zpair)
    start(rcopy(foreign.at[core], half(core, zlo, y, 1), gs.at[1], gr.at[1], znext))
    own = item(core, zlo, y)
    send_on(own, 2, yabove)
    send_on(own, 3, ybelow)
    start(rcopy(q_hbm.at[:, 1 - core], qbuf.at[:, :, qcol], qsem.at[0], qsem.at[1], mate))
    weights_on(2)

    order = [
        zlo * 4 + y, zother * 4 + y, zlo * 4 + ydn, zlo * 4 + yup,
        zother * 4 + ydn, zother * 4 + yup, zlo * 4 + yfar, zother * 4 + yfar,
    ]

    def gathered(n):
        if n == 1:
            got = half(core, zother, y, 1)
            arrived(got, gr.at[1])
            send_on(got, 4, yabove)
            send_on(got, 5, ybelow)
            pass_on(got, 1)
            got = half(core, zother, y, 0)
            arrived(got, gr.at[0])
            pass_on(got, 0)
            weights_on(1)
        elif n == 2:
            got = item(core, zlo, ydn)
            arrived(got, gr.at[2])
            send_on(half(core, zlo, ydn, 0), 6, yabove)
            send_on(half(core, zlo, ydn, 0), 7, zpair)
            pass_on(got, 2)
            got = item(core, zlo, yup)
            arrived(got, gr.at[3])
            send_on(half(core, zlo, yup, 1), 8, ybelow)
            send_on(half(core, zlo, yup, 0), 9, zpair)
            pass_on(got, 3)
            weights_on(2)
        elif n == 4:
            below, above = half(core, zother, ydn, 1), half(core, zother, yup, 1)
            arrived(below, gr.at[4])
            arrived(above, gr.at[5])
            lower = core == 0
            source = jnp.where(lower, ydn, yup)
            target = at_ctx(zlo, jnp.where(lower, yup, ydn))
            send_on(half(core, zother, source, 1), 10, target)
            pass_on(below, 4)
            pass_on(above, 5)
            got = half(core, zlo, yfar, 0)
            arrived(got, gr.at[6])
            send_on(got, 11, zpair)
            pass_on(got, 6)
            got = half(core, zlo, yfar, 1)
            arrived(got, gr.at[8])
            pass_on(got, 8)
            weights_on(1)
        elif n == 5:
            got = half(core, zother, ydn, 0)
            arrived(got, gr.at[7])
            pass_on(got, 7)
            got = half(core, zother, yup, 0)
            arrived(got, gr.at[9])
            pass_on(got, 9)
            weights_on(2)
        elif n == 7:
            got = half(core, zother, yfar, 1)
            arrived(got, gr.at[10])
            pass_on(got, 10)
            got = half(core, zother, yfar, 0)
            arrived(got, gr.at[11])
            pass_on(got, 11)

    def ready(n):
        what = 1 - core
        if n == 1:
            arrived(half(what, zother, y, 1), dr.at[1])
            arrived(half(what, zother, y, 0), dr.at[0])
        elif n == 2:
            arrived(item(what, zlo, ydn), dr.at[2])
        elif n == 3:
            arrived(item(what, zlo, yup), dr.at[3])
        elif n == 4:
            arrived(half(what, zother, ydn, 1), dr.at[4])
            arrived(half(what, zother, ydn, 0), dr.at[7])
        elif n == 5:
            arrived(half(what, zother, yup, 1), dr.at[5])
            arrived(half(what, zother, yup, 0), dr.at[9])
        elif n == 6:
            arrived(half(what, zlo, yfar, 0), dr.at[6])
            arrived(half(what, zlo, yfar, 1), dr.at[8])
        elif n == 7:
            arrived(half(what, zother, yfar, 1), dr.at[10])
            arrived(half(what, zother, yfar, 0), dr.at[11])
        for part in range(2):
            span = order[n] * 2 + part
            vt[span, :HD] = kv[1, span].T

    vt[:, HD:] = jnp.ones((16, 16, SPAN), bf16)

    score_scale = math.log2(math.e) / math.sqrt(HD)

    def fold(scores):
        return jnp.max(scores.reshape(SPAN // 8, 8, 256), axis=0)

    def scores_of(place, tile, key_span):
        keys = kv[0, key_span]
        keys = jnp.concatenate([keys, keys], axis=1)
        parts = [
            jnp.dot(keys[h * 256 : (h + 1) * 256], qt[place, tile], preferred_element_type=f32) for h in range(2)
        ]
        return jnp.concatenate(parts, axis=0)

    def start_of(span):
        row = posall[span // 2, pl.ds((span % 2) * (SPAN // 128), 1), :]
        return jnp.concatenate([row, row], axis=1)

    own_spans = (2 * ctx, 2 * ctx + 1)

    def prepare(place):
        for tile in range(4):
            way, hh = tile // 2, tile % 2
            rows = qbuf[way * 4 + visits[place][way]]
            stack = jnp.concatenate(
                [rows[:, (hh * 4 + h) * HD : (hh * 4 + h + 1) * HD] for h in range(4)], axis=0
            )
            qf = stack.astype(f32).T * score_scale
            hi = qf.astype(bf16)
            lo = (qf - hi.astype(f32)).astype(bf16)
            qt[place, tile] = jnp.concatenate([hi, lo], axis=0)

    left, right, far = (x + 3) % 4, (x + 1) % 4, (x + 2) % 4
    visits = ((left, right), (far, far), (right, left), (x, x))

    own_starts = [start_of(span) for span in own_spans]

    def own_span(tile, i):
        way = tile // 2
        return 2 * ctx + (way if i == 0 else 1 - way)

    def arriving_span(tile, i):
        return order[i // 2 % 8] * 2 + i % 2

    def other_span(tile, i):
        return (2 * ctx + i) % 16

    def masked(place, tile, s):
        key_at = lax.broadcasted_iota(jnp.int32, (SPAN, 256), 0)
        row_at = lax.broadcasted_iota(jnp.int32, (SPAN, 256), 1) % ROWS
        return jnp.where(key_at <= row_at + (visits[place][tile // 2] * 128 + core * ROWS), s, NEG)

    def product(place, tile, span, slot):
        r = jnp.dot(vt[span], p_sc[slot], preferred_element_type=f32)[: HD + 8]
        acc[place, tile] = acc[place, tile] * a_sc[slot] + r

    def opening(place, span, own=False):
        s = scores_of(place, 0, span)
        if own:
            s = masked(place, 0, s)
        s_sc[0] = s
        t_sc[0] = fold(s)

    def units(place, span_at, i, own=False, first=False, last=False):
        for tile in range(4):
            cur, nxt = tile % 2, (tile + 1) % 2
            after, ai = (tile + 1) % 4, i + (tile + 1) // 4
            before, bi = (tile + 3) % 4, i - (1 if tile == 0 else 0)
            ends = last and tile == 3
            top = jnp.max(t_sc[cur], axis=0, keepdims=True)
            old = m_sc[place, tile]
            if own:
                new = offset = jnp.maximum(old, top)
            else:
                visible = start_of(span_at(tile, i)) < own_starts[tile // 2]
                bias = jnp.where(visible, 0.0, NEG).astype(f32)
                new = jnp.maximum(old, top + bias)
                offset = new - bias
            m_sc[place, tile] = new
            if not ends:
                s = scores_of(place, after, span_at(after, ai))
                if own and tile < 3:
                    s = masked(place, after, s)
            if not (first and tile == 0):
                product(place, before, span_at(before, bi), nxt)
            a_sc[cur] = jnp.exp2(old - new)
            tops = None
            for sub in range(4):
                rows = slice(sub * 128, (sub + 1) * 128)
                if not ends:
                    s_sc[nxt, rows] = s[rows]
                    t = jnp.max(s[rows].reshape(16, 8, 256), axis=0)
                    tops = t if tops is None else jnp.maximum(tops, t)
                p_sc[cur, rows] = jnp.exp2(s_sc[cur, rows] - offset).astype(bf16)
            if not ends:
                t_sc[nxt] = tops

    def attend_own(place):
        prepare(place)
        for tile in range(4):
            m_sc[place, tile] = jnp.full((1, 256), NEG, f32)
            acc[place, tile] = jnp.zeros((HD + 8, 256), f32)
        opening(place, own_span(0, 0), True)
        units(place, own_span, 0, own=True, first=True)
        units(place, own_span, 1, last=True)
        product(place, 3, own_span(3, 1), 1)

    def attend_arriving():
        ready(0)
        attend_own(0)
        attend_own(1)
        gathered(1)
        attend_own(2)
        for i in range(1, 8):
            src = posall.at[(ctx + 8 - i) % 8]
            rcopy(src, src, ps.at[0], pr.at[i - 1], mate).wait_recv()
        gathered(2)
        attend_own(3)
        ready(1)
        opening(0, arriving_span(0, 2))
        for n in range(1, 8):
            if n in (2, 3, 5):
                gathered({2: 4, 3: 5, 5: 7}[n])
            if n < 7:
                ready(n + 1)
            units(0, arriving_span, 2 * n, first=n == 1)
            units(0, arriving_span, 2 * n + 1, last=n == 7)
        product(0, 3, arriving_span(3, 15), 1)
        attended(0)

    def attend_others(place, between=None):
        opening(place, other_span(0, 2))
        p_sc[1] = jnp.zeros((SPAN, 256), bf16)
        a_sc[1] = jnp.ones((1, 256), f32)

        for low, high in ((1, 8),) if between is None else ((1, 4), (4, 8)):

            @pl.loop(low, high)
            def _(n):
                units(place, other_span, 2 * n)
                units(place, other_span, 2 * n + 1)

            if high == 4:
                between()

        product(place, 3, other_span(3, 15), 1)
        attended(place)

    def attended(place):
        for tile in range(4):
            way, hh = tile // 2, tile % 2
            out = (acc[place, tile, :HD] / acc[place, tile, HD : HD + 1]).T.astype(bf16)
            for h in range(4):
                head = hh * 4 + h
                att[place, way * ROWS : (way + 1) * ROWS, head * HD : (head + 1) * HD] = out[
                    h * ROWS : (h + 1) * ROWS
                ]

    def projected(place, cols):
        r = jnp.dot(att[place, :, :512], wbuf[0, :, cols], preferred_element_type=f32)
        return r + jnp.dot(att[place, :, 512:], wbuf[1, :, cols], preferred_element_type=f32)

    mine = zhi == 0

    def across(step, place, chunks=range(A_CHUNKS)):
        for chunk in chunks:
            piece = pl.ds(chunk * A_PER, A_PER)
            if step == 0:
                weights_here(chunk)
            if step > 0:
                for way in range(2):
                    arrived(recv.at[way, step - 1, :, piece], xr.at[way, step - 1, chunk])

            for t in range(A_PER // A_TILE):
                cols = pl.ds(chunk * A_PER + t * A_TILE, A_TILE)
                r = projected(place, cols)
                up, down = r[:ROWS], r[ROWS:]
                if step > 0:
                    up += recv[0, step - 1, :, cols].astype(f32)
                    down += recv[1, step - 1, :, cols].astype(f32)
                if step < 3:
                    send[0, step, :, cols] = up.astype(bf16)
                    send[1, step, :, cols] = down.astype(bf16)
                else:
                    summed[:, cols] = jnp.where(mine, up, down)
                    fin[:, cols] = jnp.where(mine, down, up).astype(bf16)

            if step < 3:
                for way, dev in ((0, xup), (1, xdn)):
                    start(
                        rcopy(
                            send.at[way, step, :, piece], recv.at[way, step, :, piece],
                            xs.at[way, step, chunk], xr.at[way, step, chunk], dev,
                        )
                    )
            else:
                start(rcopy(fin.at[:, piece], zrecv.at[:, piece], zs.at[chunk], zr.at[chunk], zmate))

    def begin(ring, step, place):
        weights_here(*((5, 6) if ring == 0 else (6, 7)))

        for t in range(B_COLS // B_TILE):
            cols = pl.ds(t * B_TILE, B_TILE)
            r = projected(place, pl.ds(A_COLS + ring * B_COLS + t * B_TILE, B_TILE))
            bown[ring, step, :, cols] = jnp.where(mine, r[:ROWS], r[ROWS:])
            zsend[ring, step, :, cols] = jnp.where(mine, r[ROWS:], r[:ROWS]).astype(bf16)

        start(
            rcopy(
                zsend.at[ring, step], zgot.at[ring, step], bzs.at[ring, step], bzr.at[ring, step], zmate
            )
        )

    def finish(ring, step):
        arrived(zgot.at[ring, step], bzr.at[ring, step])
        if step > 0:
            arrived(brecv.at[ring, step - 1], bxr.at[ring, step - 1])

        @pl.loop(0, B_COLS // TILE)
        def _(t):
            cols = pl.ds(pl.multiple_of(t * TILE, TILE), TILE)
            v = bown[ring, step, :, cols] + zgot[ring, step, :, cols].astype(f32)
            if step > 0:
                v += brecv[ring, step - 1, :, cols].astype(f32)
            if step < 3:
                bsend[ring, step, :, cols] = v.astype(bf16)
            else:
                summed[:, pl.ds(pl.multiple_of(A_COLS + ring * B_COLS + t * TILE, TILE), TILE)] = v

        if step < 3:
            ahead = (x + jnp.where((zhi + ring) % 2 == 0, 1, 3)) % 4
            start(
                rcopy(
                    bsend.at[ring, step], brecv.at[ring, step], bxs.at[ring, step], bxr.at[ring, step],
                    at_tp(zhi, ahead, core),
                )
            )

    loads[5].wait()
    qother = qbuf.at[:, :, pl.ds(pl.multiple_of((1 - core) * 512, 512), 512)]
    arrived(qother, qsem.at[1])
    attend_arriving()
    weights_on(8)
    loads[6].wait()
    begin(0, 0, 0)
    across(0, 0)
    begin(1, 2, 0)
    attend_others(1)
    finish(0, 0)
    begin(0, 1, 1)
    begin(1, 1, 1)
    across(1, 1, range(2))
    attend_others(2, lambda: across(1, 1, range(2, A_CHUNKS)))
    begin(1, 0, 2)
    begin(0, 2, 2)
    finish(0, 1)

    def meanwhile():
        across(2, 2, range(3))
        finish(1, 0)

    attend_others(3, meanwhile)
    begin(0, 3, 3)
    begin(1, 3, 3)
    finish(0, 2)
    finish(1, 1)
    across(2, 2, range(3, A_CHUNKS))
    across(3, 3, range(3))
    finish(1, 2)
    across(3, 3, range(3, A_CHUNKS))
    finish(0, 3)
    finish(1, 3)

    loads[7].wait()
    stores = []

    def hand_out(n, low, high, crossed):
        for t in range(low, high, TILE):
            cols = slice(t, t + TILE)
            total = summed[:, cols] + res[:, cols].astype(f32)
            if crossed:
                total += zrecv[:, cols].astype(f32)
            summed[:, cols] = total
        piece = pl.ds(low, high - low)
        copy = pltpu.make_async_copy(summed.at[:, piece], total_hbm.at[:, piece], tsem.at[n])
        copy.start()
        stores.append(copy)

    hand_out(A_CHUNKS, A_COLS, WIDTH, False)
    for chunk in range(A_CHUNKS):
        arrived(zrecv.at[:, pl.ds(chunk * A_PER, A_PER)], zr.at[chunk])
        hand_out(chunk, chunk * A_PER, (chunk + 1) * A_PER, True)
    for copy in stores:
        copy.wait()
    for copy in started:
        copy.wait_send()


def norm_kernel(scale_ref, total_ref, gain_ref, hidden_ref, clipped_ref):
    squares = jnp.zeros((NORM_ROWS, TILE), f32)
    for t in range(0, WIDTH, TILE):
        total = total_ref[:, t : t + TILE]
        hidden_ref[:, t : t + TILE] = total.astype(bf16)
        squares += total * total
    inv_rms = lax.rsqrt(jnp.sum(squares, axis=1, keepdims=True) * (1.0 / WIDTH) + 1e-5)
    limit = 448.0 * scale_ref[0]
    per = TILE // 128
    for t in range(WIDTH // TILE):
        cols = slice(t * TILE, (t + 1) * TILE)
        gain = jnp.concatenate([gain_ref[t * per + i : t * per + i + 1, :] for i in range(per)], axis=1)
        value = total_ref[:, cols] * inv_rms * gain
        clipped_ref[:, cols] = jnp.minimum(jnp.maximum(value, -limit), limit).astype(bf16)


def shards(queries, context_keys, context_values, positions, out_weight, residual_in, norm_gain, static_scale):
    dma = pltpu.SemaphoreType.DMA
    anywhere = pl.BlockSpec(memory_space=pl.ANY)
    total = pl.pallas_call(
        kernel,
        out_shape=jax.ShapeDtypeStruct((ROWS, WIDTH), f32),
        in_specs=[anywhere] * 6,
        out_specs=anywhere,
        scratch_shapes=[
            pltpu.VMEM((2, 512, WIDTH), bf16),
            pltpu.VMEM((2, 16, SPAN, HD), bf16),
            pltpu.VMEM((2, 1, SPAN, HD), bf16),
            pltpu.VMEM((16, HD + 16, SPAN), bf16),
            pltpu.VMEM((8, ROWS, 1024), bf16),
            pltpu.VMEM((8, 8, 128), jnp.int32),
            pltpu.VMEM((4, 4, 2 * HD, 256), bf16),
            pltpu.VMEM((4, 4, HD + 8, 256), f32),
            pltpu.VMEM((4, 4, 1, 256), f32),
            pltpu.VMEM((2, 1, 256), f32),
            pltpu.VMEM((2, 8, 256), f32),
            pltpu.VMEM((2, SPAN, 256), f32),
            pltpu.VMEM((2, SPAN, 256), bf16),
            pltpu.VMEM((4, 2 * ROWS, 1024), bf16),
            pltpu.VMEM((2, 3, ROWS, A_COLS), bf16),
            pltpu.VMEM((2, 3, ROWS, A_COLS), bf16),
            pltpu.VMEM((2, 4, ROWS, B_COLS), bf16),
            pltpu.VMEM((2, 4, ROWS, B_COLS), bf16),
            pltpu.VMEM((2, 4, ROWS, B_COLS), f32),
            pltpu.VMEM((2, 3, ROWS, B_COLS), bf16),
            pltpu.VMEM((2, 3, ROWS, B_COLS), bf16),
            pltpu.VMEM((ROWS, A_COLS), bf16),
            pltpu.VMEM((ROWS, A_COLS), bf16),
            pltpu.VMEM((ROWS, WIDTH), f32),
            pltpu.VMEM((ROWS, WIDTH), bf16),
            dma((8,)), dma((A_CHUNKS + 1,)), dma((2,)), dma((2, 8)), dma((12,)), dma((12,)), dma((12,)), dma((12,)), dma((7,)), dma((7,)),
            dma((2, 3, A_CHUNKS)), dma((2, 3, A_CHUNKS)), dma((2, 4)), dma((2, 4)), dma((2, 3)), dma((2, 3)),
            dma((A_CHUNKS,)), dma((A_CHUNKS,)),
        ],
        compiler_params=pltpu.CompilerParams(
            collective_id=0, has_side_effects=True, vmem_limit_bytes=62 * 1024 * 1024
        ),
    )(
        queries.reshape(8, 2, ROWS, 512),
        context_keys.reshape(2, SPAN, 1024),
        context_values.reshape(2, SPAN, 1024),
        positions.reshape(8, 128),
        out_weight,
        residual_in,
    )
    out = jax.ShapeDtypeStruct((ROWS, WIDTH), bf16)
    rows = pl.BlockSpec((NORM_ROWS, WIDTH), lambda i: (i, 0))
    return pl.pallas_call(
        norm_kernel,
        grid=(ROWS // NORM_ROWS,),
        out_shape=(out, out),
        in_specs=[
            pl.BlockSpec(memory_space=pltpu.SMEM),
            rows,
            pl.BlockSpec((WIDTH // 128, 128), lambda i: (0, 0)),
        ],
        out_specs=(rows, rows),
    )(static_scale, total, norm_gain.reshape(WIDTH // 128, 128))


def solution(mesh):
    return jax.shard_map(
        shards,
        mesh=mesh,
        in_specs=(
            P("ctx", "tp"),
            P("ctx", None),
            P("ctx", None),
            P("ctx"),
            P("tp", None),
            P(("ctx", "tp"), None),
            P(),
            P(),
        ),
        out_specs=(P(("ctx", "tp"), None), P(("ctx", "tp"), None)),
        check_vma=False,
    )
```

```python
import math

import jax
import jax.numpy as jnp
from jax import lax
from jax.experimental import pallas as pl
from jax.experimental.pallas import tpu as pltpu
from jax.sharding import PartitionSpec as P

HD = 128
SPAN = 512
ROWS = 64
WIDTH = 8192
TILE = 512
NORM_PIECES = 8
A_TILE = 1024
B_TILE = 768
A_COLS = 5120
A_CHUNKS = 5
A_PER = A_COLS // A_CHUNKS
Z_PIECES = A_COLS // TILE
B_COLS = (WIDTH - A_COLS) // 2
NEG = -1e30
MESH = pl.DeviceIdType.MESH
bf16 = jnp.bfloat16
f32 = jnp.float32


def kernel(
    q_hbm, k_hbm, v_hbm, pos_hbm, w_hbm, res_hbm,
    total_hbm,
    wbuf, kv, foreign, vt, qbuf, posall, qt, acc, m_sc, a_sc, t_sc, s_sc, p_sc, att,
    send, recv, zsend, zgot, bown, bsend, brecv, fin, zrecv, summed, res,
    lsem, tsem, qsem, wsem, gs, gr, ds, dr, ps, pr, xs, xr, bzs, bzr, bxs, bxr, zs, zr,
):
    ctx = lax.axis_index("ctx")
    tp = lax.axis_index("tp")
    zlo, y = ctx // 4, ctx % 4
    zhi, x, core = tp // 8, (tp // 2) % 4, tp % 2
    group = tp // 2
    yup, ydn, yfar = (y + 1) % 4, (y + 3) % 4, (y + 2) % 4
    zother = 1 - zlo

    def at_ctx(zl, yy):
        return (zl * 4 + yy, tp)

    def at_tp(zh, xx, cc):
        return (ctx, zh * 8 + xx * 2 + cc)

    mate = at_tp(zhi, x, 1 - core)
    xup, xdn = at_tp(zhi, (x + 1) % 4, core), at_tp(zhi, (x + 3) % 4, core)
    zmate = at_tp(1 - zhi, x, core)
    zpair = at_ctx(zother, y)
    znext = (zother * 4 + y, (1 - zhi) * 8 + x * 2 + core)
    yabove, ybelow = at_ctx(zlo, yup), at_ctx(zlo, ydn)

    def rcopy(src, dst, ssem, rsem, dev):
        return pltpu.make_async_remote_copy(
            src_ref=src, dst_ref=dst, send_sem=ssem, recv_sem=rsem, device_id=dev, device_id_type=MESH
        )

    def heads(g):
        return pl.ds(pl.multiple_of(g * HD, HD), HD)

    far_group = (1 - zhi) * 4 + x
    qcol = pl.ds(pl.multiple_of(core * 512, 512), 512)
    loads = []
    for n, (source, target) in enumerate((
        (k_hbm.at[:, :, heads(group)], kv.at[0, pl.ds(2 * ctx, 2)]),
        (v_hbm.at[:, :, heads(group)], kv.at[1, pl.ds(2 * ctx, 2)]),
        (k_hbm.at[pl.ds(1, 1), :, heads(far_group)], foreign.at[0]),
        (v_hbm.at[pl.ds(1, 1), :, heads(far_group)], foreign.at[1]),
        (pos_hbm, posall.at[ctx]),
        (q_hbm.at[:, core], qbuf.at[:, :, qcol]),
        (w_hbm, wbuf.at[core]),
        (res_hbm, res),
    )):
        copy = pltpu.make_async_copy(source, target, lsem.at[n])
        copy.start()
        loads.append(copy)

    barrier = pltpu.get_barrier_semaphore()
    peers = [mate, xup, xdn, zmate, znext] + [((ctx + i) % 8, tp) for i in range(1, 8)]
    for dev in peers:
        pl.semaphore_signal(barrier, inc=1, device_id=dev, device_id_type=MESH)
    pl.semaphore_wait(barrier, len(peers))

    def item(what, zl, yy):
        return kv.at[what, pl.ds((zl * 4 + yy) * 2, 2)]

    def half(what, zl, yy, part):
        return kv.at[what, pl.ds((zl * 4 + yy) * 2 + part, 1)]

    started = []

    def start(copy):
        copy.start()
        started.append(copy)

    waiting = [5, 6, 0, 1, 2, 3, 4, 7]

    def weights_on(count):
        for _ in range(count):
            if waiting:
                n = waiting.pop(0)
                piece = pl.ds(n * 1024, 1024)
                start(rcopy(w_hbm.at[:, piece], wbuf.at[core, :, piece], wsem.at[0, n], wsem.at[1, n], mate))

    here = set()

    def weights_here(*pieces):
        for n in pieces:
            if n not in here:
                here.add(n)
                arrived(wbuf.at[1 - core, :, pl.ds(n * 1024, 1024)], wsem.at[1, n])

    def send_on(ref, n, dev):
        start(rcopy(ref, ref, gs.at[n], gr.at[n], dev))

    def arrived(ref, sem):
        rcopy(ref, ref, gs.at[0], sem, mate).wait_recv()

    def pass_on(ref, n):
        start(rcopy(ref, ref, ds.at[n], dr.at[n], mate))

    loads[4].wait()
    for i in range(1, 8):
        start(rcopy(posall.at[ctx], posall.at[ctx], ps.at[i - 1], pr.at[i - 1], ((ctx + i) % 8, tp)))
    for n in range(4):
        loads[n].wait()
    first = half(core, zlo, y, 0)
    send_on(first, 0, zpair)
    start(rcopy(foreign.at[core], half(core, zlo, y, 1), gs.at[1], gr.at[1], znext))
    own = item(core, zlo, y)
    send_on(own, 2, yabove)
    send_on(own, 3, ybelow)
    start(rcopy(q_hbm.at[:, 1 - core], qbuf.at[:, :, qcol], qsem.at[0], qsem.at[1], mate))
    weights_on(2)

    order = [
        zlo * 4 + y, zother * 4 + y, zlo * 4 + ydn, zlo * 4 + yup,
        zother * 4 + ydn, zother * 4 + yup, zlo * 4 + yfar, zother * 4 + yfar,
    ]

    def gathered(n):
        if n == 1:
            got = half(core, zother, y, 1)
            arrived(got, gr.at[1])
            send_on(got, 4, yabove)
            send_on(got, 5, ybelow)
            pass_on(got, 1)
            got = half(core, zother, y, 0)
            arrived(got, gr.at[0])
            pass_on(got, 0)
            weights_on(1)
        elif n == 2:
            got = item(core, zlo, ydn)
            arrived(got, gr.at[2])
            send_on(half(core, zlo, ydn, 0), 6, yabove)
            send_on(half(core, zlo, ydn, 0), 7, zpair)
            pass_on(got, 2)
            got = item(core, zlo, yup)
            arrived(got, gr.at[3])
            send_on(half(core, zlo, yup, 1), 8, ybelow)
            send_on(half(core, zlo, yup, 0), 9, zpair)
            pass_on(got, 3)
            weights_on(2)
        elif n == 4:
            below, above = half(core, zother, ydn, 1), half(core, zother, yup, 1)
            arrived(below, gr.at[4])
            arrived(above, gr.at[5])
            lower = core == 0
            source = jnp.where(lower, ydn, yup)
            target = at_ctx(zlo, jnp.where(lower, yup, ydn))
            send_on(half(core, zother, source, 1), 10, target)
            pass_on(below, 4)
            pass_on(above, 5)
            got = half(core, zlo, yfar, 0)
            arrived(got, gr.at[6])
            send_on(got, 11, zpair)
            pass_on(got, 6)
            got = half(core, zlo, yfar, 1)
            arrived(got, gr.at[8])
            pass_on(got, 8)
            weights_on(1)
        elif n == 5:
            got = half(core, zother, ydn, 0)
            arrived(got, gr.at[7])
            pass_on(got, 7)
            got = half(core, zother, yup, 0)
            arrived(got, gr.at[9])
            pass_on(got, 9)
            weights_on(2)
        elif n == 7:
            got = half(core, zother, yfar, 1)
            arrived(got, gr.at[10])
            pass_on(got, 10)
            got = half(core, zother, yfar, 0)
            arrived(got, gr.at[11])
            pass_on(got, 11)

    def ready(n):
        what = 1 - core
        if n == 1:
            arrived(half(what, zother, y, 1), dr.at[1])
            arrived(half(what, zother, y, 0), dr.at[0])
        elif n == 2:
            arrived(item(what, zlo, ydn), dr.at[2])
        elif n == 3:
            arrived(item(what, zlo, yup), dr.at[3])
        elif n == 4:
            arrived(half(what, zother, ydn, 1), dr.at[4])
            arrived(half(what, zother, ydn, 0), dr.at[7])
        elif n == 5:
            arrived(half(what, zother, yup, 1), dr.at[5])
            arrived(half(what, zother, yup, 0), dr.at[9])
        elif n == 6:
            arrived(half(what, zlo, yfar, 0), dr.at[6])
            arrived(half(what, zlo, yfar, 1), dr.at[8])
        elif n == 7:
            arrived(half(what, zother, yfar, 1), dr.at[10])
            arrived(half(what, zother, yfar, 0), dr.at[11])
        for part in range(2):
            span = order[n] * 2 + part
            vt[span, :HD] = kv[1, span].T

    vt[:, HD:] = jnp.ones((16, 16, SPAN), bf16)

    score_scale = math.log2(math.e) / math.sqrt(HD)

    def fold(scores):
        return jnp.max(scores.reshape(SPAN // 8, 8, 256), axis=0)

    def scores_of(place, tile, key_span):
        keys = kv[0, key_span]
        keys = jnp.concatenate([keys, keys], axis=1)
        parts = [
            jnp.dot(keys[h * 256 : (h + 1) * 256], qt[place, tile], preferred_element_type=f32) for h in range(2)
        ]
        return jnp.concatenate(parts, axis=0)

    def start_of(span):
        row = posall[span // 2, pl.ds((span % 2) * (SPAN // 128), 1), :]
        return jnp.concatenate([row, row], axis=1)

    own_spans = (2 * ctx, 2 * ctx + 1)

    def prepare(place):
        for tile in range(4):
            way, hh = tile // 2, tile % 2
            rows = qbuf[way * 4 + visits[place][way]]
            stack = jnp.concatenate(
                [rows[:, (hh * 4 + h) * HD : (hh * 4 + h + 1) * HD] for h in range(4)], axis=0
            )
            qf = stack.astype(f32).T * score_scale
            hi = qf.astype(bf16)
            lo = (qf - hi.astype(f32)).astype(bf16)
            qt[place, tile] = jnp.concatenate([hi, lo], axis=0)

    left, right, far = (x + 3) % 4, (x + 1) % 4, (x + 2) % 4
    visits = ((left, right), (far, far), (right, left), (x, x))

    own_starts = [start_of(span) for span in own_spans]

    def own_span(tile, i):
        way = tile // 2
        return 2 * ctx + (way if i == 0 else 1 - way)

    def arriving_span(tile, i):
        return order[i // 2 % 8] * 2 + i % 2

    def other_span(tile, i):
        return (2 * ctx + i) % 16

    def masked(place, tile, s):
        key_at = lax.broadcasted_iota(jnp.int32, (SPAN, 256), 0)
        row_at = lax.broadcasted_iota(jnp.int32, (SPAN, 256), 1) % ROWS
        return jnp.where(key_at <= row_at + (visits[place][tile // 2] * 128 + core * ROWS), s, NEG)

    def product(place, tile, span, slot):
        r = jnp.dot(vt[span], p_sc[slot], preferred_element_type=f32)[: HD + 8]
        acc[place, tile] = acc[place, tile] * a_sc[slot] + r

    def opening(place, span, own=False, base=0):
        s = scores_of(place, 0, span)
        if own:
            s = masked(place, 0, s)
        s_sc[base] = s
        t_sc[base] = fold(s)

    def units(place, span_at, i, own=False, first=False, last=False, base=0):
        for tile in range(4):
            cur, nxt = base + tile % 2, base + (tile + 1) % 2
            after, ai = (tile + 1) % 4, i + (tile + 1) // 4
            before, bi = (tile + 3) % 4, i - (1 if tile == 0 else 0)
            ends = last and tile == 3
            top = jnp.max(t_sc[cur], axis=0, keepdims=True)
            old = m_sc[place, tile]
            if own:
                new = offset = jnp.maximum(old, top)
            else:
                visible = start_of(span_at(tile, i)) < own_starts[tile // 2]
                bias = jnp.where(visible, 0.0, NEG).astype(f32)
                new = jnp.maximum(old, top + bias)
                offset = new - bias
            m_sc[place, tile] = new
            if not ends:
                s = scores_of(place, after, span_at(after, ai))
                if own and tile < 3:
                    s = masked(place, after, s)
            if not (first and tile == 0):
                product(place, before, span_at(before, bi), nxt)
            a_sc[cur] = jnp.exp2(old - new)
            tops = None
            for sub in range(4):
                rows = slice(sub * 128, (sub + 1) * 128)
                if not ends:
                    s_sc[nxt, rows] = s[rows]
                    t = jnp.max(s[rows].reshape(16, 8, 256), axis=0)
                    tops = t if tops is None else jnp.maximum(tops, t)
                p_sc[cur, rows] = jnp.exp2(s_sc[cur, rows] - offset).astype(bf16)
            if not ends:
                t_sc[nxt] = tops

    def attend_own(place, base=0):
        prepare(place)
        for tile in range(4):
            m_sc[place, tile] = jnp.full((1, 256), NEG, f32)
            acc[place, tile] = jnp.zeros((HD + 8, 256), f32)
        opening(place, own_span(0, 0), True, base)
        units(place, own_span, 0, own=True, first=True, base=base)
        units(place, own_span, 1, last=True, base=base)
        product(place, 3, own_span(3, 1), base + 1)

    def attend_arriving():
        ready(0)
        attend_own(0)
        attend_own(1)
        gathered(1)
        attend_own(2)
        for i in range(1, 8):
            src = posall.at[(ctx + 8 - i) % 8]
            rcopy(src, src, ps.at[0], pr.at[i - 1], mate).wait_recv()
        gathered(2)
        ready(1)
        opening(0, arriving_span(0, 2))
        for n in range(1, 8):
            if n == 2:
                attend_own(3, 2)
            if n in (2, 3, 5):
                gathered({2: 4, 3: 5, 5: 7}[n])
            if n < 7:
                ready(n + 1)
            units(0, arriving_span, 2 * n, first=n == 1)
            units(0, arriving_span, 2 * n + 1, last=n == 7)
        product(0, 3, arriving_span(3, 15), 1)
        attended(0)

    def attend_others(place, between=None):
        opening(place, other_span(0, 2))
        p_sc[1] = jnp.zeros((SPAN, 256), bf16)
        a_sc[1] = jnp.ones((1, 256), f32)

        for low, high in ((1, 8),) if between is None else ((1, 4), (4, 8)):

            @pl.loop(low, high)
            def _(n):
                units(place, other_span, 2 * n)
                units(place, other_span, 2 * n + 1)

            if high == 4:
                between()

        product(place, 3, other_span(3, 15), 1)
        attended(place)

    def attended(place):
        for tile in range(4):
            way, hh = tile // 2, tile % 2
            out = (acc[place, tile, :HD] / acc[place, tile, HD : HD + 1]).T.astype(bf16)
            for h in range(4):
                head = hh * 4 + h
                att[place, way * ROWS : (way + 1) * ROWS, head * HD : (head + 1) * HD] = out[
                    h * ROWS : (h + 1) * ROWS
                ]

    def projected(place, cols):
        r = jnp.dot(att[place, :, :512], wbuf[0, :, cols], preferred_element_type=f32)
        return r + jnp.dot(att[place, :, 512:], wbuf[1, :, cols], preferred_element_type=f32)

    mine = zhi == 0

    def across(step, place, chunks=range(A_CHUNKS)):
        for chunk in chunks:
            piece = pl.ds(chunk * A_PER, A_PER)
            if step == 0:
                weights_here(chunk)
            if step > 0:
                for way in range(2):
                    arrived(recv.at[way, step - 1, :, piece], xr.at[way, step - 1, chunk])

            tile = A_TILE if step < 3 else TILE
            for t in range(A_PER // tile):
                cols = pl.ds(chunk * A_PER + t * tile, tile)
                r = projected(place, cols)
                up, down = r[:ROWS], r[ROWS:]
                if step > 0:
                    up += recv[0, step - 1, :, cols].astype(f32)
                    down += recv[1, step - 1, :, cols].astype(f32)
                if step < 3:
                    send[0, step, :, cols] = up.astype(bf16)
                    send[1, step, :, cols] = down.astype(bf16)
                else:
                    summed[:, cols] = jnp.where(mine, up, down)
                    fin[:, cols] = jnp.where(mine, down, up).astype(bf16)
                    n = chunk * (A_PER // TILE) + t
                    start(rcopy(fin.at[:, cols], zrecv.at[:, cols], zs.at[n], zr.at[n], zmate))

            if step < 3:
                for way, dev in ((0, xup), (1, xdn)):
                    start(
                        rcopy(
                            send.at[way, step, :, piece], recv.at[way, step, :, piece],
                            xs.at[way, step, chunk], xr.at[way, step, chunk], dev,
                        )
                    )

    def begin(ring, step, place):
        weights_here(*((5, 6) if ring == 0 else (6, 7)))

        @pl.loop(0, B_COLS // B_TILE)
        def _(t):
            cols = pl.ds(pl.multiple_of(t * B_TILE, B_TILE), B_TILE)
            r = projected(
                place, pl.ds(pl.multiple_of(A_COLS + ring * B_COLS + t * B_TILE, 256), B_TILE)
            )
            bown[ring, step, :, cols] = jnp.where(mine, r[:ROWS], r[ROWS:])
            zsend[ring, step, :, cols] = jnp.where(mine, r[ROWS:], r[:ROWS]).astype(bf16)

        start(
            rcopy(
                zsend.at[ring, step], zgot.at[ring, step], bzs.at[ring, step], bzr.at[ring, step], zmate
            )
        )

    def finish(ring, step):
        arrived(zgot.at[ring, step], bzr.at[ring, step])
        if step > 0:
            arrived(brecv.at[ring, step - 1], bxr.at[ring, step - 1])

        @pl.loop(0, B_COLS // TILE)
        def _(t):
            cols = pl.ds(pl.multiple_of(t * TILE, TILE), TILE)
            v = bown[ring, step, :, cols] + zgot[ring, step, :, cols].astype(f32)
            if step > 0:
                v += brecv[ring, step - 1, :, cols].astype(f32)
            if step < 3:
                bsend[ring, step, :, cols] = v.astype(bf16)
            else:
                summed[:, pl.ds(pl.multiple_of(A_COLS + ring * B_COLS + t * TILE, TILE), TILE)] = v

        if step < 3:
            ahead = (x + jnp.where((zhi + ring) % 2 == 0, 1, 3)) % 4
            start(
                rcopy(
                    bsend.at[ring, step], brecv.at[ring, step], bxs.at[ring, step], bxr.at[ring, step],
                    at_tp(zhi, ahead, core),
                )
            )

    loads[5].wait()
    qother = qbuf.at[:, :, pl.ds(pl.multiple_of((1 - core) * 512, 512), 512)]
    arrived(qother, qsem.at[1])
    attend_arriving()
    weights_on(8)
    loads[6].wait()
    begin(0, 0, 0)
    across(0, 0)
    begin(1, 2, 0)
    attend_others(1)
    finish(0, 0)
    begin(0, 1, 1)
    begin(1, 1, 1)
    across(1, 1, range(2))
    attend_others(2, lambda: across(1, 1, range(2, A_CHUNKS)))
    begin(1, 0, 2)
    begin(0, 2, 2)
    finish(0, 1)

    def meanwhile():
        across(2, 2, range(1))
        finish(1, 0)
        across(2, 2, range(1, 3))

    attend_others(3, meanwhile)
    begin(0, 3, 3)
    begin(1, 3, 3)
    finish(0, 2)
    finish(1, 1)
    across(2, 2, range(3, A_CHUNKS))
    across(3, 3, range(3))
    finish(1, 2)
    across(3, 3, range(3, A_CHUNKS))
    finish(0, 3)
    finish(1, 3)

    loads[7].wait()
    stores = []

    def hand_out(n, low, high, crossed):
        for t in range(low, high, TILE):
            cols = slice(t, t + TILE)
            total = summed[:, cols] + res[:, cols].astype(f32)
            if crossed:
                total += zrecv[:, cols].astype(f32)
            summed[:, cols] = total
        piece = pl.ds(low, high - low)
        copy = pltpu.make_async_copy(summed.at[:, piece], total_hbm.at[:, piece], tsem.at[n])
        copy.start()
        stores.append(copy)

    hand_out(Z_PIECES, A_COLS, WIDTH, False)
    for n in range(Z_PIECES):
        arrived(zrecv.at[:, pl.ds(n * TILE, TILE)], zr.at[n])
        hand_out(n, n * TILE, (n + 1) * TILE, True)
    for copy in stores:
        copy.wait()
    for copy in started:
        copy.wait_send()


def norm_kernel(
    scale_ref, total_hbm, gain_ref, hidden_hbm, clipped_hbm, total_ref, hidden_ref, clipped_ref, in_sem, h_sem, c_sem
):
    per = WIDTH // NORM_PIECES

    def piece(n):
        return pl.ds(n * per, per)

    reads = [
        pltpu.make_async_copy(total_hbm.at[:, piece(n)], total_ref.at[:, piece(n)], in_sem.at[n])
        for n in range(NORM_PIECES)
    ]
    writes = []

    def write(source, target, sem, n):
        copy = pltpu.make_async_copy(source.at[:, piece(n)], target.at[:, piece(n)], sem.at[n])
        copy.start()
        writes.append(copy)

    for copy in reads:
        copy.start()
    squares = jnp.zeros((ROWS, 128), f32)
    for n in range(NORM_PIECES):
        reads[n].wait()
        for t in range(n * per, (n + 1) * per, 128):
            total = total_ref[:, t : t + 128]
            hidden_ref[:, t : t + 128] = total.astype(bf16)
            squares += total * total
        write(hidden_ref, hidden_hbm, h_sem, n)
    inv_rms = lax.rsqrt(jnp.sum(squares, axis=1, keepdims=True) * (1.0 / WIDTH) + 1e-5)
    inv_rms = jnp.broadcast_to(inv_rms, (ROWS, 128))
    limit = 448.0 * scale_ref[0]
    for n in range(NORM_PIECES):
        for t in range(n * per, (n + 1) * per, 128):
            value = total_ref[:, t : t + 128] * inv_rms * gain_ref[t // 128 : t // 128 + 1, :]
            clipped_ref[:, t : t + 128] = jnp.minimum(jnp.maximum(value, -limit), limit).astype(bf16)
        write(clipped_ref, clipped_hbm, c_sem, n)
    for copy in writes:
        copy.wait()


def shards(queries, context_keys, context_values, positions, out_weight, residual_in, norm_gain, static_scale):
    dma = pltpu.SemaphoreType.DMA
    anywhere = pl.BlockSpec(memory_space=pl.ANY)
    total = pl.pallas_call(
        kernel,
        out_shape=jax.ShapeDtypeStruct((ROWS, WIDTH), f32),
        in_specs=[anywhere] * 6,
        out_specs=anywhere,
        scratch_shapes=[
            pltpu.VMEM((2, 512, WIDTH), bf16),
            pltpu.VMEM((2, 16, SPAN, HD), bf16),
            pltpu.VMEM((2, 1, SPAN, HD), bf16),
            pltpu.VMEM((16, HD + 16, SPAN), bf16),
            pltpu.VMEM((8, ROWS, 1024), bf16),
            pltpu.VMEM((8, 8, 128), jnp.int32),
            pltpu.VMEM((4, 4, 2 * HD, 256), bf16),
            pltpu.VMEM((4, 4, HD + 8, 256), f32),
            pltpu.VMEM((4, 4, 1, 256), f32),
            pltpu.VMEM((4, 1, 256), f32),
            pltpu.VMEM((4, 8, 256), f32),
            pltpu.VMEM((4, SPAN, 256), f32),
            pltpu.VMEM((4, SPAN, 256), bf16),
            pltpu.VMEM((4, 2 * ROWS, 1024), bf16),
            pltpu.VMEM((2, 3, ROWS, A_COLS), bf16),
            pltpu.VMEM((2, 3, ROWS, A_COLS), bf16),
            pltpu.VMEM((2, 4, ROWS, B_COLS), bf16),
            pltpu.VMEM((2, 4, ROWS, B_COLS), bf16),
            pltpu.VMEM((2, 4, ROWS, B_COLS), f32),
            pltpu.VMEM((2, 3, ROWS, B_COLS), bf16),
            pltpu.VMEM((2, 3, ROWS, B_COLS), bf16),
            pltpu.VMEM((ROWS, A_COLS), bf16),
            pltpu.VMEM((ROWS, A_COLS), bf16),
            pltpu.VMEM((ROWS, WIDTH), f32),
            pltpu.VMEM((ROWS, WIDTH), bf16),
            dma((8,)), dma((Z_PIECES + 1,)), dma((2,)), dma((2, 8)), dma((12,)), dma((12,)), dma((12,)), dma((12,)), dma((7,)), dma((7,)),
            dma((2, 3, A_CHUNKS)), dma((2, 3, A_CHUNKS)), dma((2, 4)), dma((2, 4)), dma((2, 3)), dma((2, 3)),
            dma((Z_PIECES,)), dma((Z_PIECES,)),
        ],
        compiler_params=pltpu.CompilerParams(
            collective_id=0, has_side_effects=True, vmem_limit_bytes=62 * 1024 * 1024
        ),
    )(
        queries.reshape(8, 2, ROWS, 512),
        context_keys.reshape(2, SPAN, 1024),
        context_values.reshape(2, SPAN, 1024),
        positions.reshape(8, 128),
        out_weight,
        residual_in,
    )
    out = jax.ShapeDtypeStruct((ROWS, WIDTH), bf16)
    return pl.pallas_call(
        norm_kernel,
        out_shape=(out, out),
        in_specs=[pl.BlockSpec(memory_space=pltpu.SMEM), anywhere, pl.BlockSpec(memory_space=pltpu.VMEM)],
        out_specs=(anywhere, anywhere),
        scratch_shapes=[
            pltpu.VMEM((ROWS, WIDTH), f32),
            pltpu.VMEM((ROWS, WIDTH), bf16),
            pltpu.VMEM((ROWS, WIDTH), bf16),
            dma((NORM_PIECES,)), dma((NORM_PIECES,)), dma((NORM_PIECES,)),
        ],
    )(static_scale, total, norm_gain.reshape(WIDTH // 128, 128))


def solution(mesh):
    return jax.shard_map(
        shards,
        mesh=mesh,
        in_specs=(
            P("ctx", "tp"),
            P("ctx", None),
            P("ctx", None),
            P("ctx"),
            P("tp", None),
            P(("ctx", "tp"), None),
            P(),
            P(),
        ),
        out_specs=(P(("ctx", "tp"), None), P(("ctx", "tp"), None)),
        check_vma=False,
    )
```
